128 devices in a mesh: fsdp: 32 (over z, x_hi, y), tp: 4 (over x_lo, core).
Axes of the slice: x: 4 (x_hi: 2, x_lo: 2; x = x_hi * 2 + x_lo), y: 4, z: 4, core: 2. Of those that a mesh axis runs over, the one named last changes fastest.
Arguments:
- base_o: bfloat16 [2, 8192, 8192], P(None, 'tp', 'fsdp'), may hold values from -0.0625 to 0.0625
- base_down: bfloat16 [2, 28672, 8192], P(None, 'tp', 'fsdp'), may hold values from -0.03125 to 0.03125
- factor_a_o: bfloat16 [2, 64, 4, 2048], P(None, None, None, 'fsdp'), may hold values from -0.0625 to 0.0625
- factor_b_o: bfloat16 [2, 8192, 64], P(None, 'fsdp'), may hold values from -1.1953125 to 1.1953125
- factor_a_down: bfloat16 [2, 64, 4, 7168], P(None, None, None, 'fsdp'), may hold values from -0.03125 to 0.03125
- factor_b_down: bfloat16 [2, 8192, 64], P(None, 'fsdp'), may hold values from -1.1953125 to 1.1953125
- magnitude_o: float32 [2, 8192], P(None, 'fsdp'), may hold values from 30 to 300
- magnitude_down: float32 [2, 8192], P(None, 'fsdp'), may hold values from 30 to 300
Outputs:
- merged_o: bfloat16 [2, 8192, 8192], P(None, 'tp', 'fsdp')
- merged_down: bfloat16 [2, 28672, 8192], P(None, 'tp', 'fsdp')
The draws below stay inside these ranges and needn't reach their ends.
All inputs are finite; a program needn't handle non-finite values.
Results may differ from the reference program's by a relative error of at most 0.001.
Values may be sent and summed in bfloat16 or wider, within the bound.
No kernel may reach another device: no remote copies, remote signals or barrier semaphores. Data moves between devices by JAX's collectives and lax.ppermute only.
A program may use at most 128 MiB of HBM per device.

```python
import math
import jax
import jax.numpy as jnp
from jax import lax

D = 8192
FF = 28672
R = 64
LAYERS = 2
N_TP = 4


def level_of(rng, dims, cuts, smallest, top_value):
    def one(dim, shards_of):
        steps = jax.random.uniform(jax.random.fold_in(jax.random.fold_in(rng, 6), dim), (shards_of,), jnp.float32, smallest / len(cuts), top_value / len(cuts))
        return jnp.repeat(jnp.exp(steps), dims[dim] // shards_of).reshape((-1,) + (1,) * (len(dims) - dim - 1))

    level = one(*cuts[0])
    for cut in cuts[1:]:
        level = level * one(*cut)
    return level


def noise(stream_key, extent, width, reach, split=(), dtype=jnp.bfloat16):
    gain = level_of(stream_key, extent, split, -0.22, 0.18) if split else 1.0
    drawn = jax.random.normal(stream_key, extent, jnp.float32) * width * gain
    return jnp.minimum(jnp.maximum(drawn, -reach), reach).astype(dtype)


def setup_inputs(seed: int = 0) -> dict:
    seeds = jax.random.split(jax.random.key(seed), 9)
    return {
        "base_o": noise(seeds[0], (LAYERS, D, D), D ** -0.5, 0.0625, ((1, 4), (2, 32))),
        "base_down": noise(seeds[1], (LAYERS, FF, D), FF ** -0.5, 0.03125, ((1, 4), (2, 32))),
        "factor_a_o": noise(seeds[2], (LAYERS, R, N_TP, D // N_TP), D ** -0.5, 0.0625, ((3, 32),)),
        "factor_b_o": noise(seeds[3], (LAYERS, D, R), 0.2, 1.1953125, ((1, 32),)),
        "factor_a_down": noise(seeds[4], (LAYERS, R, N_TP, FF // N_TP), FF ** -0.5, 0.03125, ((3, 32),)),
        "factor_b_down": noise(seeds[5], (LAYERS, D, R), 0.2, 1.1953125, ((1, 32),)),
        "magnitude_o": jnp.clip(jnp.exp(math.log(300.0) - 2.3025851 * jax.random.uniform(seeds[6], (LAYERS, D), jnp.float32) ** level_of(seeds[6], (LAYERS, D), ((1, 32),), -0.2, 0.2)), 30.0, 300.0),
        "magnitude_down": jnp.clip(jnp.exp(math.log(300.0) - 2.3025851 * jax.random.uniform(seeds[7], (LAYERS, D), jnp.float32) ** level_of(seeds[7], (LAYERS, D), ((1, 32),), -0.2, 0.2)), 30.0, 300.0),
    }


def refresh(base, factor_a, factor_b, magnitude):
    full_a = factor_a.reshape(factor_a.shape[0], factor_a.shape[1], -1)

    def single(items):
        base_layer, a_layer, b_layer, m_layer = items
        delta = jnp.dot(a_layer.T, b_layer.T, preferred_element_type=jnp.float32)
        summed = base_layer.astype(jnp.float32) + 0.25 * delta
        square = lax.optimization_barrier(jnp.sum(summed * summed, axis=0))
        return (m_layer[None, :] * summed * lax.rsqrt(square + 1e-06)[None, :]).astype(jnp.bfloat16)
    return lax.map(single, (base, full_a, factor_b, magnitude))

def reference(base_o, base_down, factor_a_o, factor_b_o, factor_a_down, factor_b_down, magnitude_o, magnitude_down):
    merged_o = refresh(base_o, factor_a_o, factor_b_o, magnitude_o)
    merged_down = refresh(base_down, factor_a_down, factor_b_down, magnitude_down)
    return (merged_o, merged_down)
```

```python
import functools

import jax
import jax.numpy as jnp
import numpy as np
from jax import lax
from jax.experimental import pallas as pl
from jax.experimental.pallas import tpu as pltpu
from jax.sharding import Mesh
from jax.sharding import PartitionSpec as P

AXES = ("z", "xh", "y", "xl", "c")
SHAPE = (4, 2, 4, 2, 2)
TP = ("xl", "c")
FSDP = ("z", "xh", "y")
STEPS = (0, -1, 1, 2)
HALF = 144
DOWN = 224
ATTN = 64
TAIL = DOWN - HALF
COLS = 256
BF16 = jnp.bfloat16
F32 = jnp.float32


def pairs(target):
    index = np.arange(128).reshape(SHAPE)
    return [(int(index[k]), int(index[tuple(target(*k))])) for k in np.ndindex(*SHAPE)]


def along_y(k):
    return pairs(lambda z, h, y, l, c: (z, h, (y - k) % 4, l, c))


def along_z(k):
    return pairs(lambda z, h, y, l, c: ((z - k) % 4, h, y, l, c))


ACROSS_X = pairs(lambda z, h, y, l, c: (z, 1 - h, y, 1 - l, c))
OTHER_CORE = pairs(lambda z, h, y, l, c: (z, h, y, l, 1 - c))
OTHER_CHIP = pairs(lambda z, h, y, l, c: (z, h, y, 1 - l, c))
OTHER_BOTH = pairs(lambda z, h, y, l, c: (z, h, y, 1 - l, 1 - c))


def permute(x, table):
    return lax.ppermute(x, AXES, table)


def packed(factor_a_o, factor_a_down, column):
    def rows(factor):
        own = lax.dynamic_index_in_dim(factor, column, 2, keepdims=False)
        return own.reshape(128, own.shape[-1]).T

    return jnp.concatenate([rows(factor_a_down), rows(factor_a_o)], 0)


def shard_of(dz, dy, h):
    z, xh, y = (lax.axis_index(name) for name in FSDP)
    far = lax.rem(z + (dz + 4), 4)
    side = lax.rem(xh + h, 2)
    return far * 8 + side * 4 + lax.rem(y + (dy + 4), 4)


def shards(half, piece):
    for j, h in np.ndindex(4, 2):
        if half == 0:
            yield shard_of(STEPS[piece], STEPS[j], int(h))
        else:
            yield shard_of(STEPS[j], STEPS[piece], int(h))


def start_of(f, rows, offset):
    return pl.multiple_of(f * rows + offset, 16)


def weights_kernel(bo_ref, bd_ref, wo_ref, wd_ref):
    for b_ref, w_ref in ((bo_ref, wo_ref), (bd_ref, wd_ref)):
        none = jnp.zeros((64, COLS), BF16)
        quarter = jnp.asarray(0.25, F32)
        b = [(b_ref[l].astype(F32) * quarter).astype(BF16) for l in range(2)]
        w_ref[0:64, 0:COLS] = b[0]
        w_ref[0:64, COLS:] = none
        w_ref[64:128, 0:COLS] = none
        w_ref[64:128, COLS:] = b[1]


def deltas(half, a, wo_ref, wd_ref, d_ref):
    if half == 0:
        d_ref[...] = jnp.dot(
            a.reshape(8 * HALF, 128), wd_ref[...], preferred_element_type=F32
        )
    else:
        d_ref[: 8 * TAIL] = jnp.dot(
            a[:, :TAIL].reshape(8 * TAIL, 128), wd_ref[...], preferred_element_type=F32
        )
        d_ref[8 * TAIL :] = jnp.dot(
            a[:, TAIL:].reshape(8 * ATTN, 128), wo_ref[...], preferred_element_type=F32
        )


def parts(half, s, f):
    if half == 0:
        yield 1, start_of(f, DOWN, 0), s * HALF, HALF
    else:
        yield 1, start_of(f, DOWN, HALF), s * TAIL, TAIL
        yield 0, start_of(f, ATTN, 0), 8 * TAIL + s * ATTN, ATTN


def squares_kernel(half, pieces, *refs):
    n = len(pieces)
    a_refs = refs[:n]
    wo_ref, wd_ref, base_o_ref, base_d_ref, out_ref, d_ref = refs[n:]
    acc = {(p, l): jnp.zeros((8, COLS), F32) for p in range(2) for l in range(2)}
    for piece, a_ref in zip(pieces, a_refs):
        deltas(half, a_ref[...], wo_ref, wd_ref, d_ref)
        for s, f in enumerate(shards(half, piece)):
            for p, row, at, rows in parts(half, s, f):
                base_ref = (base_o_ref, base_d_ref)[p]
                for l in range(2):
                    summed = (
                        base_ref[l, pl.ds(row, rows), :].astype(F32)
                        + d_ref[at : at + rows, l * COLS : (l + 1) * COLS]
                    )
                    acc[p, l] += jnp.sum((summed * summed).reshape(rows // 8, 8, COLS), 0)
    for p in range(2):
        for l in range(2):
            out_ref[p, l] = acc[p, l]


def merge_kernel(*refs):
    a_refs = refs[:8]
    (wo_ref, wd_ref, base_o_ref, base_d_ref, square_ref, mag_o_ref, mag_d_ref) = refs[8:15]
    out_o_ref, out_d_ref, buf_o, buf_d, d_ref, sem = refs[15:]
    scale = {}
    for p, mag_ref in enumerate((mag_o_ref, mag_d_ref)):
        for l in range(2):
            scale[p, l] = mag_ref[l : l + 1, :] * lax.rsqrt(square_ref[p, l : l + 1, :] + 1e-06)
    outs = ((buf_o, out_o_ref), (buf_d, out_d_ref))
    for half in range(2):
        for piece in range(4):
            deltas(half, a_refs[half * 4 + piece][...], wo_ref, wd_ref, d_ref)
            for s, f in enumerate(shards(half, piece)):
                for p, row, at, rows in parts(half, s, f):
                    base_ref = (base_o_ref, base_d_ref)[p]
                    buf, out = outs[p]
                    for l in range(2):
                        summed = (
                            base_ref[l, pl.ds(row, rows), :].astype(F32)
                            + d_ref[at : at + rows, l * COLS : (l + 1) * COLS]
                        )
                        buf[l, pl.ds(row, rows), :] = (summed * scale[p, l]).astype(BF16)
                    pltpu.make_async_copy(
                        buf.at[:, pl.ds(row, rows), :], out.at[:, pl.ds(row, rows), :], sem.at[p]
                    ).start()
    for p, (buf, out) in enumerate(outs):
        pltpu.make_async_copy(buf, out, sem.at[p]).wait()


VMEM = pl.BlockSpec(memory_space=pltpu.VMEM)
ANY = pl.BlockSpec(memory_space=pl.ANY)


def call(kernel, outs, n_in, out_specs, scratch=(), cost=None):
    return pl.pallas_call(
        kernel,
        out_shape=outs,
        in_specs=[VMEM] * n_in,
        out_specs=out_specs,
        scratch_shapes=list(scratch),
        cost_estimate=cost,
    )


def local(
    base_o,
    base_down,
    factor_a_o,
    factor_b_o,
    factor_a_down,
    factor_b_down,
    magnitude_o,
    magnitude_down,
):
    column = lax.axis_index(TP)
    own = packed(factor_a_o, factor_a_down, column)
    sent = packed(factor_a_o, factor_a_down, lax.rem(column + 2, 4))
    w_shape = jax.ShapeDtypeStruct((128, 2 * COLS), BF16)
    wo, wd = call(weights_kernel, (w_shape, w_shape), 2, (VMEM, VMEM))(
        jnp.swapaxes(factor_b_o, 1, 2), jnp.swapaxes(factor_b_down, 1, 2)
    )
    got = permute(sent, ACROSS_X)
    first = jnp.stack([own[:HALF], got[:HALF]])
    second = jnp.stack([own[HALF:], got[HALF:]])
    first = jnp.concatenate([first] + [permute(first, along_y(k)) for k in STEPS[1:]])
    second = jnp.concatenate([second] + [permute(second, along_z(k)) for k in STEPS[1:]])
    pieces = [
        [first] + [permute(first, along_z(k)) for k in STEPS[1:]],
        [second] + [permute(second, along_y(k)) for k in STEPS[1:]],
    ]
    partial = []
    for half in range(2):
        for group in ((0,), (1, 2, 3)):
            cost = pl.CostEstimate(
                flops=len(group) * 2 * 1152 * 128 * 512,
                bytes_accessed=len(group) * 2 * 1152 * 512,
                transcendentals=0,
            )
            partial.append(
                call(
                    functools.partial(squares_kernel, half, group),
                    jax.ShapeDtypeStruct((2, 2, 8, COLS), F32),
                    len(group) + 4,
                    VMEM,
                    (pltpu.VMEM((8 * HALF, 2 * COLS), F32),),
                    cost,
                )(*[pieces[half][g] for g in group], wo, wd, base_o, base_down)
            )
    square = jnp.sum(sum(partial), axis=2)
    square = (
        square
        + permute(square, OTHER_CORE)
        + permute(square, OTHER_CHIP)
        + permute(square, OTHER_BOTH)
    )
    return tuple(
        pl.pallas_call(
            merge_kernel,
            out_shape=(
                jax.ShapeDtypeStruct(base_o.shape, BF16),
                jax.ShapeDtypeStruct(base_down.shape, BF16),
            ),
            in_specs=[VMEM] * 15,
            out_specs=(ANY, ANY),
            scratch_shapes=[
                pltpu.VMEM(base_o.shape, BF16),
                pltpu.VMEM(base_down.shape, BF16),
                pltpu.VMEM((8 * HALF, 2 * COLS), F32),
                pltpu.SemaphoreType.DMA((2,)),
            ],
        )(
            *pieces[0],
            *pieces[1],
            wo,
            wd,
            base_o,
            base_down,
            square,
            magnitude_o,
            magnitude_down,
        )
    )


def solution(mesh):
    finer = Mesh(mesh.devices.reshape(SHAPE), AXES)
    in_specs = (
        P(None, TP, FSDP),
        P(None, TP, FSDP),
        P(None, None, None, FSDP),
        P(None, FSDP, None),
        P(None, None, None, FSDP),
        P(None, FSDP, None),
        P(None, FSDP),
        P(None, FSDP),
    )
    out_specs = (P(None, TP, FSDP), P(None, TP, FSDP))
    return jax.shard_map(local, mesh=finer, in_specs=in_specs, out_specs=out_specs, check_vma=False)
```
